16 devices in a mesh: dp: 1, tp: 16 (over x, y, z, core).
Axes of the slice: x: 2, y: 2, z: 2, core: 2. Of those that a mesh axis runs over, the one named last changes fastest.
Arguments:
- x: bfloat16 [2048, 8192], P(('dp', 'tp'))
- dy: bfloat16 [2048, 8192], P(('dp', 'tp'))
- gate: bfloat16 [2048, 49152], P('dp', 'tp')
- up: bfloat16 [2048, 49152], P('dp', 'tp')
- w_gate: bfloat16 [8192, 49152], P(None, 'tp')
- w_up: bfloat16 [8192, 49152], P(None, 'tp')
- w_down: bfloat16 [49152, 8192], P('tp')
Outputs:
- output 1: bfloat16 [2048, 8192], P(('dp', 'tp'))
- output 2: bfloat16 [8192, 49152], P('dp', 'tp')
- output 3: bfloat16 [8192, 49152], P('dp', 'tp')
- output 4: bfloat16 [49152, 8192], P(('dp', 'tp'))
All inputs are finite; a program needn't handle non-finite values.
Results may differ from the reference program's by a relative error of at most 0.012.
Values are sent between devices in bfloat16 or wider.
A program may use at most 2 GiB of HBM per device.

```python
import jax
import jax.numpy as jnp

ROWS = 2048
D = 8192
FF = 49152


def act(gate, up):
    return jax.nn.silu(gate) * up


def setup_inputs(seed: int = 0, part: int = 0) -> dict:
    kx, ky, ka, kb, kg, ku, kd = jax.random.split(jax.random.key(seed), 7)
    kx, ky, ka, kb = (jax.random.fold_in(k, part) for k in (kx, ky, ka, kb))
    drawn = {
        "x": jax.random.normal(kx, (ROWS, D), jnp.float32),
        "dy": jax.random.normal(ky, (ROWS, D), jnp.float32),
        "gate": jax.random.normal(ka, (ROWS, FF), jnp.float32),
        "up": jax.random.normal(kb, (ROWS, FF), jnp.float32),
        "w_gate": jax.random.normal(kg, (D, FF), jnp.float32) * D**-0.5,
        "w_up": jax.random.normal(ku, (D, FF), jnp.float32) * D**-0.5,
        "w_down": jax.random.normal(kd, (FF, D), jnp.float32) * FF**-0.5,
    }
    return {k: v.astype(jnp.bfloat16) for k, v in drawn.items()}


def reference(x, dy, gate, up, w_gate, w_up, w_down):
    hidden, back = jax.vjp(act, gate.astype(jnp.float32), up.astype(jnp.float32))
    d_hidden = jnp.dot(dy, w_down.T, preferred_element_type=jnp.float32)
    d_gate, d_up = (g.astype(jnp.bfloat16) for g in back(d_hidden))
    dx = jnp.dot(d_gate, w_gate.T, preferred_element_type=jnp.float32) + jnp.dot(d_up, w_up.T, preferred_element_type=jnp.float32)
    dw_gate = jnp.dot(x.T, d_gate, preferred_element_type=jnp.float32)
    dw_up = jnp.dot(x.T, d_up, preferred_element_type=jnp.float32)
    dw_down = jnp.dot(hidden.astype(jnp.bfloat16).T, dy, preferred_element_type=jnp.float32)
    return tuple(g.astype(jnp.bfloat16) for g in (dx, dw_gate, dw_up, dw_down))
```

```python
import jax
import jax.numpy as jnp
from jax import lax
from jax.sharding import PartitionSpec as P


def act(gate, up):
    return jax.nn.silu(gate) * up


def solution(mesh):
    rows = P(("dp", "tp"), None)
    cols = P("dp", "tp")
    wcol = P(None, "tp")
    wrow = P("tp", None)

    def body(x, dy, gate, up, w_gate, w_up, w_down):
        f32, bf16 = jnp.float32, jnp.bfloat16
        dy = lax.all_gather(dy, "tp", axis=0, tiled=True)
        x = lax.all_gather(x, "tp", axis=0, tiled=True)
        hidden, back = jax.vjp(act, gate.astype(f32), up.astype(f32))
        d_hidden = lax.dot_general(dy, w_down, (((1,), (1,)), ((), ())), preferred_element_type=f32)
        d_gate, d_up = (g.astype(bf16) for g in back(d_hidden))
        nt = (((1,), (1,)), ((), ()))
        tn = (((0,), (0,)), ((), ()))
        dx = lax.dot_general(d_gate, w_gate, nt, preferred_element_type=f32)
        dx = dx + lax.dot_general(d_up, w_up, nt, preferred_element_type=f32)
        dx = lax.psum_scatter(dx.astype(bf16), "tp", scatter_dimension=0, tiled=True)
        dwd = lax.dot_general(hidden.astype(bf16), dy, tn, preferred_element_type=f32).astype(bf16)
        dwg = lax.dot_general(x, d_gate, tn, preferred_element_type=f32).astype(bf16)
        dwu = lax.dot_general(x, d_up, tn, preferred_element_type=f32).astype(bf16)
        return dx, dwg, dwu, dwd

    return jax.shard_map(
        body,
        mesh=mesh,
        in_specs=(rows, rows, cols, cols, wcol, wcol, wrow),
        out_specs=(rows, cols, cols, P(("dp", "tp"), None)),
        check_vma=False,
    )
```

```python
import jax
import jax.numpy as jnp
from jax import lax
from jax.experimental import pallas as pl
from jax.experimental.pallas import tpu as pltpu
from jax.sharding import PartitionSpec as P

f32, bf16 = jnp.float32, jnp.bfloat16
NT = (((1,), (1,)), ((), ()))
TN = (((0,), (0,)), ((), ()))

PART = (48, 48, 32)
FROM = (0, 48, 96)
AXES = ((0, 1, 2), (1, 2, 0), (2, 0, 1))
FLIPS = ((0, 0, 0), (1, 0, 0), (0, 1, 0), (0, 0, 1), (1, 1, 0), (1, 0, 1), (0, 1, 1), (1, 1, 1))
HOP = (None, (0, 0), (0, 1), (0, 2), (1, 1), (1, 2), (2, 2), (4, 2))
ROWS = 256


def slot(j, p, k):
    return pl.ds(j * ROWS + 2 * FROM[p] + k * PART[p], PART[p])


def act_grads(g, u, dh):
    s = lax.logistic(g)
    silu = g * s
    return silu * u, (dh * u) * (s + silu * (1.0 - s)), dh * silu


B1, B2, WIDE = 512, 512, 2048


def front(nd, T, D, F):
    n1, n2 = F // B1, D // B2
    steps = 4 * n1 + 3 * n2
    big = 3 * ROWS
    A1, A2 = 2 * n1, 3 * n1 + n2
    dy_at = {1: n1 - 1, 2: n1 + 4, 3: A1 + 3, 4: A1 + 8, 5: A1 + 12, 6: A1 + n2, 7: A1 + n2 + 2}
    x_at = {1: A2 - 1, 2: A2 + 2, 3: A2 + 5, 4: A2 + 8, 5: A2 + 11, 6: A2 + 14, 7: A2 + n2 + 1}

    def kern(x, dy, gate, up, wd, wg, wu, dyr, xr, hid, dg, du, dx,
             dyv, wv, gv, uv, dhv, gu, hv, dxv, send, recv, send2, recv2, ls, gs, ws, hs, xs):
        i = pl.program_id(0)
        me = lax.axis_index("tp")
        at = (me // 8, me // 4 % 2, me // 2 % 2)
        core = me % 2

        def device(flip, k=0):
            c = [1 - at[a] if flip[a] else at[a] for a in range(3)]
            return ((c[0] * 2 + c[1]) * 2 + c[2]) * 2 + (1 - core if k else core)

        def axis_flip(p, bits):
            flip = [0, 0, 0]
            for a, b in zip(AXES[p], bits):
                flip[a] = b
            return flip

        def copy(src, dst, sem):
            return pltpu.make_async_copy(src, dst, sem)

        full, own = (dyr, xr), (dy, x)

        def hop(a, j, p):
            src, along = HOP[j]
            ref = own[a].at[pl.ds(FROM[p], PART[p])] if src == 0 else full[a].at[slot(src, p, 0)]
            bits = [int(b == along) for b in range(3)]
            return pltpu.make_async_remote_copy(
                ref, full[a].at[slot(j, p, 0)], send.at[a, j, p], recv.at[a, j, p],
                device_id={"tp": device(axis_flip(p, bits))}, device_id_type=pl.DeviceIdType.MESH)

        def across(a, j, p):
            ref = own[a].at[pl.ds(FROM[p], PART[p])] if j == 0 else full[a].at[slot(j, p, 0)]
            return pltpu.make_async_remote_copy(
                ref, full[a].at[slot(j, p, 1)], send2.at[a, j, p], recv2.at[a, j, p],
                device_id={"tp": device((0, 0, 0), 1)}, device_id_type=pl.DeviceIdType.MESH)

        def begin(a):
            for p in range(3):
                across(a, 0, p).start()
            for j in (1, 2, 3):
                for p in range(3):
                    hop(a, j, p).start()

        def arrive(a, j):
            for p in range(3):
                hop(a, j, p).wait_recv()
            for later in range(4, 8):
                if HOP[later][0] == j:
                    for p in range(3):
                        hop(a, later, p).start()
            for p in range(3):
                across(a, j, p).start()

        def arrived(a, j):
            for p in range(3):
                across(a, j, p).wait_recv()

        def wdc(j, s):
            return [copy(wd.at[pl.ds(pl.multiple_of(j * B1, B1), B1)], wv.at[s], ws.at[s, 0])]

        def wgu(j, s):
            r = pl.ds(pl.multiple_of(j * B2, B2), B2)
            return [copy(w.at[r], wv.at[s, :, pl.ds(n * F, F)], ws.at[s, n]) for n, w in ((0, wg), (1, wu))]

        def kept(j, row):
            out = []
            for p in range(3):
                for k in range(2):
                    r = pl.ds(pl.multiple_of(device(axis_flip(p, FLIPS[j]), k) * 128 + FROM[p], 16), PART[p])
                    d = pl.ds(row + 2 * FROM[p] + k * PART[p], PART[p])
                    out += [copy(gate.at[r], gv.at[d], gs.at[0, row // ROWS]), copy(up.at[r], uv.at[d], gs.at[1, row // ROWS])]
            return out

        def kept_wait(row):
            d = pl.ds(row, ROWS)
            copy(gate.at[pl.ds(0, ROWS)], gv.at[d], gs.at[0, row // ROWS]).wait()
            copy(up.at[pl.ds(0, ROWS)], uv.at[d], gs.at[1, row // ROWS]).wait()

        def start(cs):
            for c in cs:
                c.start()

        def wait(cs):
            for c in cs:
                c.wait()

        def other(j):
            return [copy(dyr.at[slot(j, p, 1)], dyv.at[slot(j, p, 1)], ls.at[4 + p]) for p in range(3)]

        def load(j, n, row):
            return copy(dyr.at[pl.ds(j * ROWS, n * ROWS)], dyv.at[pl.ds(row, n * ROWS)], ls.at[0])

        def act(row, m, t, s, q):
            w = B1 // 2
            c = pl.ds(pl.multiple_of(t * B1 + q * w, w), w)
            r = pl.ds(row, m)
            h, g, u = act_grads(gv[r, c].astype(f32), uv[r, c].astype(f32), dhv[:m, q * w : (q + 1) * w])
            hv[s, :m, q * w : (q + 1) * w] = h.astype(bf16)
            gu[r, c] = g.astype(bf16)
            gu[r, pl.ds(pl.multiple_of(F + t * B1 + q * w, w), w)] = u.astype(bf16)

        def put_at(to, m, row, t, s):
            r, v, c = pl.ds(to, m), pl.ds(row, m), pl.ds(pl.multiple_of(t * B1, B1), B1)
            c2 = pl.ds(pl.multiple_of(F + t * B1, B1), B1)
            return [copy(hv.at[s, pl.ds(0, m)], hid.at[r, c], hs.at[s, 0]),
                    copy(gu.at[v, c], dg.at[r, c], hs.at[s, 1]),
                    copy(gu.at[v, c2], du.at[r, c], hs.at[s, 2])]

        def put_dx(j, n, t, s):
            out = []
            for b in range(n):
                for p in range(3):
                    for k in range(2):
                        r = pl.ds(pl.multiple_of(device(axis_flip(p, FLIPS[j + b]), k) * 128 + FROM[p], 16), PART[p])
                        v = pl.ds(b * ROWS + 2 * FROM[p] + k * PART[p], PART[p])
                        out.append(copy(dxv.at[s, v], dx.at[r, pl.ds(pl.multiple_of(t * WIDE, WIDE), WIDE)], xs.at[s]))
            return out

        def put_dx_wait(n, s):
            v = pl.ds(0, n * ROWS)
            copy(dxv.at[s, v], dx.at[v, pl.ds(0, WIDE)], xs.at[s]).wait()

        sl = lax.rem(i, 2)
        nx = 1 - sl

        events = {}

        def once(step):
            def add(f):
                events.setdefault(step, []).append(f)
            return add

        def dispatch(at):
            if len(at) == 1:
                @pl.when(i == at[0])
                def _():
                    for f in events[at[0]]:
                        f()
            else:
                mid = len(at) // 2

                @pl.when(i < at[mid])
                def _():
                    dispatch(at[:mid])

                @pl.when(i >= at[mid])
                def _():
                    dispatch(at[mid:])

        @once(0)
        def _():
            start(wdc(0, 0))
            for p in range(3):
                copy(dy.at[pl.ds(FROM[p], PART[p])], dyv.at[slot(0, p, 0)], ls.at[1 + p]).start()
            barrier = pltpu.get_barrier_semaphore()
            peers = [device((1, 0, 0)), device((0, 1, 0)), device((0, 0, 1)), device((0, 0, 0), 1)]
            for d in peers:
                pl.semaphore_signal(barrier, 1, device_id={"tp": d}, device_id_type=pl.DeviceIdType.MESH)
            pl.semaphore_wait(barrier, 4)
            begin(0)
            start(kept(0, 0))
            for p in range(3):
                copy(dy.at[pl.ds(FROM[p], PART[p])], dyv.at[slot(0, p, 0)], ls.at[1 + p]).wait()
                copy(dyv.at[slot(0, p, 0)], dyr.at[slot(0, p, 0)], ls.at[1 + p]).start()
            arrived(0, 0)
            start(other(0))
            wait(other(0))
            kept_wait(0)

        @once(1)
        def _():
            start(kept(1, ROWS))
            for p in range(3):
                copy(dyv.at[slot(0, p, 0)], dyr.at[slot(0, p, 0)], ls.at[1 + p]).wait()
            for p in range(3):
                copy(x.at[pl.ds(FROM[p], PART[p])], dyv.at[pl.ds(2 * ROWS + FROM[p], PART[p])], ls.at[1 + p]).start()

        @once(3)
        def _():
            for p in range(3):
                copy(x.at[pl.ds(FROM[p], PART[p])], dyv.at[pl.ds(2 * ROWS + FROM[p], PART[p])], ls.at[1 + p]).wait()
            for p in range(3):
                copy(dyv.at[pl.ds(2 * ROWS + FROM[p], PART[p])], xr.at[slot(0, p, 0)], ls.at[1 + p]).start()

        @once(n1 - 2)
        def _():
            for p in range(3):
                copy(dyv.at[pl.ds(2 * ROWS + FROM[p], PART[p])], xr.at[slot(0, p, 0)], ls.at[1 + p]).wait()

        def on_arrival(a, j):
            @once((dy_at, x_at)[a][j])
            def _():
                arrive(a, j)
                if (a, j) == (0, 1):
                    for p in range(3):
                        copy(dyr.at[slot(1, p, 0)], dyv.at[slot(1, p, 0)], ls.at[1 + p]).start()
                if (a, j) == (0, 4):
                    begin(1)

        for j in range(1, 8):
            on_arrival(0, j)
            on_arrival(1, j)

        @once(n1)
        def _():
            arrived(0, 1)
            start(other(1))
            kept_wait(ROWS)
            for p in range(3):
                copy(dyr.at[slot(1, p, 0)], dyv.at[slot(1, p, 0)], ls.at[1 + p]).wait()
            wait(other(1))

        def next_rows(s0, j0):
            for b in range(3):
                once(s0 + 1 + b)(lambda b=b: start(kept(j0 + b, b * ROWS)))

            @once(s0 + n2 - 4)
            def _():
                for b in range(3):
                    arrived(0, j0 + b)
                load(j0, 3, 0).start()

            @once(s0 + n2)
            def _():
                for b in range(3):
                    kept_wait(b * ROWS)
                load(j0, 3, 0).wait()

        next_rows(A1, 2)
        next_rows(A2, 5)
        dispatch(sorted(events))

        per = WIDE // B2

        def dh_step(m, row, t, prev_row, prev_t):
            wait(wdc(t, sl))
            for q in range(2):
                w = B1 // 2
                act(prev_row, m, prev_t, sl, q)
                dhv[:m, q * w : (q + 1) * w] = lax.dot_general(
                    dyv[pl.ds(row, m)], wv[sl, q * w : (q + 1) * w], NT, preferred_element_type=f32)

        def put_small(start_if, wait_if):
            @pl.when(wait_if)
            def _():
                u = i - 3
                b = u // n1
                wait(put_at(b * ROWS, ROWS, b * ROWS, u - b * n1, sl))

            @pl.when(start_if)
            def _():
                u = i - 2
                b = u // n1
                start(put_at(b * ROWS, ROWS, b * ROWS, u - b * n1, nx))

        def dx_step(m, t):
            wait(wgu(t, sl))
            dxv[t // per % 2, :m, pl.ds(pl.multiple_of(t % per * B2, B2), B2)] = lax.dot_general(
                gu[:m], wv[sl, :, : 2 * F], NT, preferred_element_type=f32).astype(bf16)

        @pl.when(i < 2 * n1)
        def _():
            t = i % n1

            @pl.when(i < 2 * n1 - 1)
            def _():
                start(wdc((i + 1) % n1, nx))

            @pl.when(i == 2 * n1 - 1)
            def _():
                start(wgu(0, nx))

            put_small(i >= 2, i >= 3)
            prev = jnp.maximum(i - 1, 0)
            dh_step(ROWS, pl.multiple_of(i // n1 * ROWS, ROWS), t, pl.multiple_of(prev // n1 * ROWS, ROWS), prev % n1)

        @pl.when((i >= A1) & (i < A1 + n2))
        def _():
            t = i - A1

            @pl.when(t < n2 - 1)
            def _():
                start(wgu(t + 1, nx))

            @pl.when(t == n2 - 1)
            def _():
                start(wdc(0, nx))

            @pl.when(t < 3)
            def _():
                put_small(t < 2, t < 3)

                @pl.when(t == 0)
                def _():
                    for q in range(2):
                        act(ROWS, ROWS, n1 - 1, sl, q)

            @pl.when((t >= per) & (t % per == 0))
            def _():
                start(put_dx(0, 2, t // per - 1, (t // per - 1) % 2))

                @pl.when(t >= 2 * per)
                def _():
                    put_dx_wait(2, t // per % 2)

            dx_step(2 * ROWS, t)

        @pl.when(i >= A1 + n2)
        def _():
            second = i >= A2 + n2
            k = i - jnp.where(second, A2 + n2, A1 + n2)
            j0 = jnp.where(second, 5 * ROWS, 2 * ROWS)

            @pl.when((k < n1 - 1) | ((k == n1 + n2 - 1) & (i < steps - 1)))
            def _():
                start(wdc(jnp.where(k < n1 - 1, k + 1, 0), nx))

            @pl.when((k >= n1 - 1) & (k < n1 + n2 - 1))
            def _():
                start(wgu(k + 1 - n1, nx))

            @pl.when((k >= 2) & (k < n1 + 3))
            def _():
                @pl.when(k >= 3)
                def _():
                    wait(put_at(pl.multiple_of(j0, ROWS), big, 0, k - 3, sl))

                @pl.when(k < n1 + 2)
                def _():
                    start(put_at(pl.multiple_of(j0, ROWS), big, 0, k - 2, nx))

            @pl.when(k < n1)
            def _():
                @pl.when(jnp.logical_not(second) & (k % per == 0) & (k <= per))
                def _():
                    last = n2 // per - 1

                    @pl.when(k == 0)
                    def _():
                        start(put_dx(0, 2, last, last % 2))
                        put_dx_wait(2, (last - 1) % 2)

                    @pl.when(k == per)
                    def _():
                        put_dx_wait(2, last % 2)

                @pl.when(second & (k % per == 0) & (k <= per))
                def _():
                    last = n2 // per - 1

                    @pl.when(k == 0)
                    def _():
                        start(put_dx(2, 3, last, last % 2))
                        put_dx_wait(3, (last - 1) % 2)

                    @pl.when(k == per)
                    def _():
                        put_dx_wait(3, last % 2)

                dh_step(big, 0, k, 0, jnp.maximum(k - 1, 0))

            @pl.when(k >= n1)
            def _():
                t = k - n1

                @pl.when(t == 0)
                def _():
                    for q in range(2):
                        act(0, big, n1 - 1, sl, q)

                @pl.when((t >= per) & (t % per == 0))
                def _():
                    g = t // per

                    @pl.when(second)
                    def _():
                        start(put_dx(5, 3, g - 1, (g - 1) % 2))

                    @pl.when(jnp.logical_not(second))
                    def _():
                        start(put_dx(2, 3, g - 1, (g - 1) % 2))

                    @pl.when(t >= 2 * per)
                    def _():
                        put_dx_wait(3, g % 2)

                dx_step(big, t)

        @pl.when(i == steps - 1)
        def _():
            last = n2 // per - 1
            start(put_dx(5, 3, last, last % 2))
            put_dx_wait(3, (last - 1) % 2)
            put_dx_wait(3, last % 2)
            for a in range(2):
                for j in range(8):
                    for p in range(3):
                        across(a, j, p).wait_send()
                        if j:
                            hop(a, j, p).wait_send()
            for j in range(8):
                arrived(1, j)

    sh = jax.ShapeDtypeStruct
    anyspec = pl.BlockSpec(memory_space=pl.ANY)
    dma = pltpu.SemaphoreType.DMA
    return pl.pallas_call(
        kern, grid=(steps,), name="front", in_specs=[anyspec] * 7, out_specs=[anyspec] * 6,
        out_shape=[sh((T, D), bf16)] * 2 + [sh((T, F), bf16)] * 3 + [sh((T, D), bf16)],
        scratch_shapes=[
            pltpu.VMEM((big, D), bf16), pltpu.VMEM((2, B1, D), bf16), pltpu.VMEM((big, F), bf16), pltpu.VMEM((big, F), bf16),
            pltpu.VMEM((big, B1), f32), pltpu.VMEM((big, 2 * F), bf16), pltpu.VMEM((2, big, B1), bf16),
            pltpu.VMEM((2, big, WIDE), bf16),
            dma((2, 8, 3)), dma((2, 8, 3)), dma((2, 8, 3)), dma((2, 8, 3)), dma((7,)), dma((2, 3)), dma((2, 2)), dma((2, 3)), dma((2,)),
        ],
        compiler_params=pltpu.CompilerParams(
            vmem_limit_bytes=62 * 2**20, dimension_semantics=("arbitrary",), collective_id=0, has_side_effects=True),
        cost_estimate=pl.CostEstimate(flops=6 * T * D * F, bytes_accessed=2 * (9 * D * F + 6 * T * D + 5 * T * F), transcendentals=T * F),
    )


def weights(T, D, F, bw=512, mt=768):
    n = D // bw

    def kern(dy, x, hid, dg, du, dwd, dwg, dwu, hv, gv, uv, blk, ws, bs):
        i = pl.program_id(0)

        def block(a, j, s):
            return pltpu.make_async_copy(a.at[:, pl.ds(pl.multiple_of(j * bw, bw), bw)], blk.at[s], bs.at[s])

        def whole(k):
            return pltpu.make_async_copy((hid, dg, du)[k], (hv, gv, uv)[k], ws.at[k])

        s = lax.rem(i, 2)

        @pl.when(i == 0)
        def _():
            block(dy, 0, 0).start()
            whole(0).start()
            whole(0).wait()

        @pl.when(i + 1 < n)
        def _():
            block(dy, i + 1, 1 - s).start()

        @pl.when((i + 1 >= n) & (i + 1 < 2 * n))
        def _():
            block(x, i + 1 - n, 1 - s).start()

        @pl.when(i == 1)
        def _():
            whole(1).start()
            whole(2).start()

        @pl.when(i < n)
        def _():
            block(dy, i, s).wait()
            for m in range(0, F, mt):
                dwd[m : m + mt, :] = lax.dot_general(
                    hv[:, m : m + mt], blk[s], TN, preferred_element_type=f32).astype(bf16)

        @pl.when(i == n)
        def _():
            whole(1).wait()
            whole(2).wait()

        @pl.when(i >= n)
        def _():
            block(x, i - n, s).wait()
            for src, dst in ((gv, dwg), (uv, dwu)):
                for m in range(0, F, mt):
                    dst[:, m : m + mt] = lax.dot_general(
                        blk[s], src[:, m : m + mt], TN, preferred_element_type=f32).astype(bf16)

    sh = jax.ShapeDtypeStruct
    dma = pltpu.SemaphoreType.DMA
    late = pl.BlockSpec((bw, F), lambda i: (jnp.maximum(i - n, 0), 0))
    return pl.pallas_call(
        kern, grid=(2 * n,), name="weights", in_specs=[pl.BlockSpec(memory_space=pl.ANY)] * 5,
        out_specs=[pl.BlockSpec((F, bw), lambda i: (0, jnp.minimum(i, n - 1))), late, late],
        out_shape=[sh((F, D), bf16), sh((D, F), bf16), sh((D, F), bf16)],
        scratch_shapes=[pltpu.VMEM((T, F), bf16)] * 3 + [pltpu.VMEM((2, T, bw), bf16), dma((3,)), dma((2,))],
        compiler_params=pltpu.CompilerParams(vmem_limit_bytes=62 * 2**20, dimension_semantics=("arbitrary",)),
        cost_estimate=pl.CostEstimate(flops=6 * T * D * F, bytes_accessed=2 * (3 * D * F + 2 * T * D + 3 * T * F), transcendentals=0),
    )


def solution(mesh):
    rows, cols = P(("dp", "tp"), None), P("dp", "tp")
    wcol, wrow = P(None, "tp"), P("tp", None)
    nd = mesh.shape["tp"]

    def body(x, dy, gate, up, w_gate, w_up, w_down):
        T, F, D = gate.shape[0], gate.shape[1], x.shape[1]
        dyr, xr, hid, dg, du, dx = front(nd, T, D, F)(x, dy, gate, up, w_down, w_gate, w_up)
        dx = lax.psum_scatter(dx, "tp", scatter_dimension=0, tiled=True)
        dwd, dwg, dwu = weights(T, D, F)(dyr, xr, hid, dg, du)
        return dx, dwg, dwu, dwd

    return jax.shard_map(
        body, mesh=mesh, in_specs=(rows, rows, cols, cols, wcol, wcol, wrow), out_specs=(rows, cols, cols, rows), check_vma=False)
```

```python
import jax
import jax.numpy as jnp
from jax import lax
from jax.experimental import pallas as pl
from jax.experimental.pallas import tpu as pltpu
from jax.sharding import PartitionSpec as P

f32, bf16 = jnp.float32, jnp.bfloat16
NT = (((1,), (1,)), ((), ()))
TN = (((0,), (0,)), ((), ()))

PART = (48, 48, 32)
FROM = (0, 48, 96)
AXES = ((0, 1, 2), (1, 2, 0), (2, 0, 1))
FLIPS = ((0, 0, 0), (1, 0, 0), (0, 1, 0), (0, 0, 1), (1, 1, 0), (1, 0, 1), (0, 1, 1), (1, 1, 1))
HOP = (None, (0, 0), (0, 1), (0, 2), (1, 1), (1, 2), (2, 2), (4, 2))
ROWS = 256


def slot(j, p, k):
    return pl.ds(j * ROWS + 2 * FROM[p] + k * PART[p], PART[p])


def act_grads(g, u, dh):
    s = lax.logistic(g)
    silu = g * s
    return silu * u, (dh * u) * (s + silu * (1.0 - s)), dh * silu


B1, B2, WIDE = 512, 1024, 1024


def front(nd, T, D, F):
    n1, n2 = F // B1, D // B2
    steps = 4 * n1 + 3 * n2
    big = 3 * ROWS
    A1, A2 = 2 * n1, 3 * n1 + n2
    dy_at = {1: n1 - 1, 2: n1 + 5, 3: A1 + 3, 4: A1 + 5, 5: A1 + n2, 6: A1 + n2 + 2, 7: A1 + n2 + 5}
    x_at = {1: A2 + 1, 2: A2 + 3, 3: A2 + 4, 4: A2 + 6, 5: A2 + 7, 6: A2 + 9, 7: A2 + 12}

    def kern(x, dy, gate, up, wd, wg, wu, dyr, xr, hid, dg, du, dx,
             dyv, wv, gv, uv, dhv, gu, hv, dxv, send, recv, send2, recv2, ls, gs, ws, hs, xs):
        i = pl.program_id(0)
        me = lax.axis_index("tp")
        at = (me // 8, me // 4 % 2, me // 2 % 2)
        core = me % 2

        def device(flip, k=0):
            c = [1 - at[a] if flip[a] else at[a] for a in range(3)]
            return ((c[0] * 2 + c[1]) * 2 + c[2]) * 2 + (1 - core if k else core)

        def axis_flip(p, bits):
            flip = [0, 0, 0]
            for a, b in zip(AXES[p], bits):
                flip[a] = b
            return flip

        def copy(src, dst, sem):
            return pltpu.make_async_copy(src, dst, sem)

        full, own = (dyr, xr), (dy, x)

        def hop(a, j, p):
            src, along = HOP[j]
            ref = own[a].at[pl.ds(FROM[p], PART[p])] if src == 0 else full[a].at[slot(src, p, 0)]
            bits = [int(b == along) for b in range(3)]
            return pltpu.make_async_remote_copy(
                ref, full[a].at[slot(j, p, 0)], send.at[a, j, p], recv.at[a, j, p],
                device_id={"tp": device(axis_flip(p, bits))}, device_id_type=pl.DeviceIdType.MESH)

        def across(a, j, p):
            ref = own[a].at[pl.ds(FROM[p], PART[p])] if j == 0 else full[a].at[slot(j, p, 0)]
            return pltpu.make_async_remote_copy(
                ref, full[a].at[slot(j, p, 1)], send2.at[a, j, p], recv2.at[a, j, p],
                device_id={"tp": device((0, 0, 0), 1)}, device_id_type=pl.DeviceIdType.MESH)

        def begin(a):
            for p in range(3):
                across(a, 0, p).start()
            for j in (1, 2, 3):
                for p in range(3):
                    hop(a, j, p).start()

        def arrive(a, j):
            for p in range(3):
                hop(a, j, p).wait_recv()
            for later in range(4, 8):
                if HOP[later][0] == j:
                    for p in range(3):
                        hop(a, later, p).start()
            for p in range(3):
                across(a, j, p).start()

        def arrived(a, j):
            for p in range(3):
                across(a, j, p).wait_recv()

        def wdc(j, s):
            r = pl.ds(pl.multiple_of(j * B1, B1), B1)
            return [copy(wd.at[r, pl.ds(h * D // 2, D // 2)], wv.at[s, pl.ds(h * B1, B1), pl.ds(0, D // 2)], ws.at[s, h])
                    for h in range(2)]

        def wgu(j, s):
            r = pl.ds(pl.multiple_of(j * B2, B2), B2)
            return [copy(w.at[r], wv.at[s, :, pl.ds(n * F, F)], ws.at[s, n]) for n, w in ((0, wg), (1, wu))]

        def kept(j, row):
            out = []
            for p in range(3):
                for k in range(2):
                    r = pl.ds(pl.multiple_of(device(axis_flip(p, FLIPS[j]), k) * 128 + FROM[p], 16), PART[p])
                    d = pl.ds(row + 2 * FROM[p] + k * PART[p], PART[p])
                    out += [copy(gate.at[r], gv.at[d], gs.at[0, row // ROWS]), copy(up.at[r], uv.at[d], gs.at[1, row // ROWS])]
            return out

        def kept_wait(row):
            d = pl.ds(row, ROWS)
            copy(gate.at[pl.ds(0, ROWS)], gv.at[d], gs.at[0, row // ROWS]).wait()
            copy(up.at[pl.ds(0, ROWS)], uv.at[d], gs.at[1, row // ROWS]).wait()

        def start(cs):
            for c in cs:
                c.start()

        def wait(cs):
            for c in cs:
                c.wait()

        def other(j):
            return [copy(dyr.at[slot(j, p, 1)], dyv.at[slot(j, p, 1)], ls.at[4 + p]) for p in range(3)]

        def load(j, n, row):
            return copy(dyr.at[pl.ds(j * ROWS, n * ROWS)], dyv.at[pl.ds(row, n * ROWS)], ls.at[0])

        def act(row, m, t, s, q):
            w = B1 // 2
            c = pl.ds(pl.multiple_of(t * B1 + q * w, w), w)
            for o in range(0, m, 128):
                r = pl.ds(row + o, 128)
                h, g, u = act_grads(gv[r, c].astype(f32), uv[r, c].astype(f32), dhv[o : o + 128, q * w : (q + 1) * w])
                hv[s, o : o + 128, q * w : (q + 1) * w] = h.astype(bf16)
                gu[r, c] = g.astype(bf16)
                gu[r, pl.ds(pl.multiple_of(F + t * B1 + q * w, w), w)] = u.astype(bf16)

        def put_at(to, m, row, t, s):
            r, v, c = pl.ds(to, m), pl.ds(row, m), pl.ds(pl.multiple_of(t * B1, B1), B1)
            c2 = pl.ds(pl.multiple_of(F + t * B1, B1), B1)
            return [copy(hv.at[s, pl.ds(0, m)], hid.at[r, c], hs.at[s, 0]),
                    copy(gu.at[v, c], dg.at[r, c], hs.at[s, 1]),
                    copy(gu.at[v, c2], du.at[r, c], hs.at[s, 2])]

        def put_dx(j, n, t, s):
            out = []
            for b in range(n):
                for p in range(3):
                    for k in range(2):
                        r = pl.ds(pl.multiple_of(device(axis_flip(p, FLIPS[j + b]), k) * 128 + FROM[p], 16), PART[p])
                        v = pl.ds(b * ROWS + 2 * FROM[p] + k * PART[p], PART[p])
                        out.append(copy(dxv.at[s, v], dx.at[r, pl.ds(pl.multiple_of(t * WIDE, WIDE), WIDE)], xs.at[s]))
            return out

        def put_dx_wait(n, s):
            v = pl.ds(0, n * ROWS)
            copy(dxv.at[s, v], dx.at[v, pl.ds(0, WIDE)], xs.at[s]).wait()

        sl = lax.rem(i, 2)
        nx = 1 - sl

        events = {}

        def once(step):
            def add(f):
                events.setdefault(step, []).append(f)
            return add

        def dispatch(at):
            if len(at) == 1:
                @pl.when(i == at[0])
                def _():
                    for f in events[at[0]]:
                        f()
            else:
                mid = len(at) // 2

                @pl.when(i < at[mid])
                def _():
                    dispatch(at[:mid])

                @pl.when(i >= at[mid])
                def _():
                    dispatch(at[mid:])

        @once(0)
        def _():
            start(wdc(0, 0))
            for p in range(3):
                copy(dy.at[pl.ds(FROM[p], PART[p])], dyv.at[slot(0, p, 0)], ls.at[1 + p]).start()
            barrier = pltpu.get_barrier_semaphore()
            peers = [device((1, 0, 0)), device((0, 1, 0)), device((0, 0, 1)), device((0, 0, 0), 1)]
            for d in peers:
                pl.semaphore_signal(barrier, 1, device_id={"tp": d}, device_id_type=pl.DeviceIdType.MESH)
            pl.semaphore_wait(barrier, 4)
            begin(0)
            start(kept(0, 0))
            for p in range(3):
                copy(dy.at[pl.ds(FROM[p], PART[p])], dyv.at[slot(0, p, 0)], ls.at[1 + p]).wait()
                copy(dyv.at[slot(0, p, 0)], dyr.at[slot(0, p, 0)], ls.at[1 + p]).start()
            arrived(0, 0)
            start(other(0))
            wait(other(0))
            kept_wait(0)

        @once(1)
        def _():
            start(kept(1, ROWS))
            for p in range(3):
                copy(dyv.at[slot(0, p, 0)], dyr.at[slot(0, p, 0)], ls.at[1 + p]).wait()
            for p in range(3):
                copy(x.at[pl.ds(FROM[p], PART[p])], dyv.at[pl.ds(2 * ROWS + FROM[p], PART[p])], ls.at[1 + p]).start()

        @once(3)
        def _():
            for p in range(3):
                copy(x.at[pl.ds(FROM[p], PART[p])], dyv.at[pl.ds(2 * ROWS + FROM[p], PART[p])], ls.at[1 + p]).wait()
            for p in range(3):
                copy(dyv.at[pl.ds(2 * ROWS + FROM[p], PART[p])], xr.at[slot(0, p, 0)], ls.at[1 + p]).start()

        @once(n1 - 2)
        def _():
            for p in range(3):
                copy(dyv.at[pl.ds(2 * ROWS + FROM[p], PART[p])], xr.at[slot(0, p, 0)], ls.at[1 + p]).wait()

        def on_arrival(a, j):
            @once((dy_at, x_at)[a][j])
            def _():
                arrive(a, j)
                if (a, j) == (0, 1):
                    for p in range(3):
                        copy(dyr.at[slot(1, p, 0)], dyv.at[slot(1, p, 0)], ls.at[1 + p]).start()
                if (a, j) == (0, 4):
                    begin(1)

        for j in range(1, 8):
            on_arrival(0, j)
            on_arrival(1, j)

        @once(n1)
        def _():
            arrived(0, 1)
            start(other(1))
            kept_wait(ROWS)
            for p in range(3):
                copy(dyr.at[slot(1, p, 0)], dyv.at[slot(1, p, 0)], ls.at[1 + p]).wait()
            wait(other(1))

        def next_rows(s0, j0):
            for b in range(3):
                once(s0 + 1 + b)(lambda b=b: start(kept(j0 + b, b * ROWS)))

            @once(s0 + n2 - 1)
            def _():
                for b in range(3):
                    arrived(0, j0 + b)
                load(j0, 3, 0).start()

            @once(s0 + n2)
            def _():
                for b in range(3):
                    kept_wait(b * ROWS)
                load(j0, 3, 0).wait()

        next_rows(A1, 2)
        next_rows(A2, 5)
        dispatch(sorted(events))

        per = WIDE // B2

        def dh_step(m, row, t, prev_row, prev_t):
            wait(wdc(t, sl))
            r, h = pl.ds(row, m), D // 2
            w = B1 if m == ROWS else B1 // 2
            for q in range(0, B1, w):
                for o in range(q, q + w, B1 // 2):
                    act(prev_row, m, prev_t, sl, o // (B1 // 2))
                dhv[:m, q : q + w] = lax.dot_general(
                    dyv[r, :h], wv[sl, q : q + w, :h], NT, preferred_element_type=f32
                ) + lax.dot_general(dyv[r, h:], wv[sl, B1 + q : B1 + q + w, :h], NT, preferred_element_type=f32)

        def put_small(start_if, wait_if):
            @pl.when(wait_if)
            def _():
                u = i - 3
                b = u // n1
                wait(put_at(b * ROWS, ROWS, b * ROWS, u - b * n1, sl))

            @pl.when(start_if)
            def _():
                u = i - 2
                b = u // n1
                start(put_at(b * ROWS, ROWS, b * ROWS, u - b * n1, nx))

        def dx_step(m, t):
            wait(wgu(t, sl))
            if m == big:
                for q in range(0, B2, B2 // 4):
                    dxv[t % 2, :, q : q + B2 // 4] = lax.dot_general(
                        gu[...], wv[sl, q : q + B2 // 4], NT, preferred_element_type=f32).astype(bf16)
            else:
                def part(q, _):
                    c = pl.ds(pl.multiple_of(q * 512, 512), 512)
                    dxv[t % 2, :m, c] = lax.dot_general(gu[:m], wv[sl, c], NT, preferred_element_type=f32).astype(bf16)
                    return 0
                lax.fori_loop(0, B2 // 512, part, 0)

        @pl.when(i < 2 * n1)
        def _():
            t = i % n1

            @pl.when(i < 2 * n1 - 1)
            def _():
                start(wdc((i + 1) % n1, nx))

            @pl.when(i == 2 * n1 - 1)
            def _():
                start(wgu(0, nx))

            put_small(i >= 2, i >= 3)
            prev = jnp.maximum(i - 1, 0)
            dh_step(ROWS, pl.multiple_of(i // n1 * ROWS, ROWS), t, pl.multiple_of(prev // n1 * ROWS, ROWS), prev % n1)

        @pl.when((i >= A1) & (i < A1 + n2))
        def _():
            t = i - A1

            @pl.when(t < n2 - 1)
            def _():
                start(wgu(t + 1, nx))

            @pl.when(t == n2 - 1)
            def _():
                start(wdc(0, nx))

            @pl.when(t < 3)
            def _():
                put_small(t < 2, t < 3)

                @pl.when(t == 0)
                def _():
                    for q in range(2):
                        act(ROWS, ROWS, n1 - 1, sl, q)

            @pl.when((t >= per) & (t % per == 0))
            def _():
                start(put_dx(0, 2, t // per - 1, (t // per - 1) % 2))

                @pl.when(t >= 2 * per)
                def _():
                    put_dx_wait(2, t // per % 2)

            dx_step(2 * ROWS, t)

        @pl.when(i >= A1 + n2)
        def _():
            second = i >= A2 + n2
            k = i - jnp.where(second, A2 + n2, A1 + n2)
            j0 = jnp.where(second, 5 * ROWS, 2 * ROWS)

            @pl.when((k < n1 - 1) | ((k == n1 + n2 - 1) & (i < steps - 1)))
            def _():
                start(wdc(jnp.where(k < n1 - 1, k + 1, 0), nx))

            @pl.when((k >= n1 - 1) & (k < n1 + n2 - 1))
            def _():
                start(wgu(k + 1 - n1, nx))

            @pl.when((k >= 2) & (k < n1 + 3))
            def _():
                @pl.when(k >= 3)
                def _():
                    wait(put_at(pl.multiple_of(j0, ROWS), big, 0, k - 3, sl))

                @pl.when(k < n1 + 2)
                def _():
                    start(put_at(pl.multiple_of(j0, ROWS), big, 0, k - 2, nx))

            @pl.when(k < n1)
            def _():
                @pl.when(jnp.logical_not(second) & (k % per == 0) & (k <= per))
                def _():
                    last = n2 // per - 1

                    @pl.when(k == 0)
                    def _():
                        start(put_dx(0, 2, last, last % 2))
                        put_dx_wait(2, (last - 1) % 2)

                    @pl.when(k == per)
                    def _():
                        put_dx_wait(2, last % 2)

                @pl.when(second & (k % per == 0) & (k <= per))
                def _():
                    last = n2 // per - 1

                    @pl.when(k == 0)
                    def _():
                        start(put_dx(2, 3, last, last % 2))
                        put_dx_wait(3, (last - 1) % 2)

                    @pl.when(k == per)
                    def _():
                        put_dx_wait(3, last % 2)

                dh_step(big, 0, k, 0, jnp.maximum(k - 1, 0))

            @pl.when(k >= n1)
            def _():
                t = k - n1

                @pl.when(t == 0)
                def _():
                    for q in range(2):
                        act(0, big, n1 - 1, sl, q)

                @pl.when((t >= per) & (t % per == 0))
                def _():
                    g = t // per

                    @pl.when(second)
                    def _():
                        start(put_dx(5, 3, g - 1, (g - 1) % 2))

                    @pl.when(jnp.logical_not(second))
                    def _():
                        start(put_dx(2, 3, g - 1, (g - 1) % 2))

                    @pl.when(t >= 2 * per)
                    def _():
                        put_dx_wait(3, g % 2)

                dx_step(big, t)

        @pl.when(i == steps - 1)
        def _():
            last = n2 // per - 1
            start(put_dx(5, 3, last, last % 2))
            put_dx_wait(3, (last - 1) % 2)
            put_dx_wait(3, last % 2)
            for a in range(2):
                for j in range(8):
                    for p in range(3):
                        across(a, j, p).wait_send()
                        if j:
                            hop(a, j, p).wait_send()
            for j in range(8):
                arrived(1, j)

    sh = jax.ShapeDtypeStruct
    anyspec = pl.BlockSpec(memory_space=pl.ANY)
    dma = pltpu.SemaphoreType.DMA
    return pl.pallas_call(
        kern, grid=(steps,), name="front", in_specs=[anyspec] * 7, out_specs=[anyspec] * 6,
        out_shape=[sh((T, D), bf16)] * 2 + [sh((T, F), bf16)] * 3 + [sh((T, D), bf16)],
        scratch_shapes=[
            pltpu.VMEM((big, D), bf16), pltpu.VMEM((2, B2, 2 * F), bf16), pltpu.VMEM((big, F), bf16), pltpu.VMEM((big, F), bf16),
            pltpu.VMEM((big, B1), f32), pltpu.VMEM((big, 2 * F), bf16), pltpu.VMEM((2, big, B1), bf16),
            pltpu.VMEM((2, big, WIDE), bf16),
            dma((2, 8, 3)), dma((2, 8, 3)), dma((2, 8, 3)), dma((2, 8, 3)), dma((7,)), dma((2, 3)), dma((2, 2)), dma((2, 3)), dma((2,)),
        ],
        compiler_params=pltpu.CompilerParams(
            vmem_limit_bytes=67_043_328, dimension_semantics=("arbitrary",), collective_id=0, has_side_effects=True),
        cost_estimate=pl.CostEstimate(flops=6 * T * D * F, bytes_accessed=2 * (9 * D * F + 6 * T * D + 5 * T * F), transcendentals=T * F),
    )


def weights(T, D, F, bw=512, mt=768):
    n = D // bw

    def kern(dy, x, hid, dg, du, dwd, dwg, dwu, hv, gv, uv, blk, ws, bs):
        i = pl.program_id(0)

        def block(a, j, s):
            return pltpu.make_async_copy(a.at[:, pl.ds(pl.multiple_of(j * bw, bw), bw)], blk.at[s], bs.at[s])

        def whole(k):
            return pltpu.make_async_copy((hid, dg, du)[k], (hv, gv, uv)[k], ws.at[k])

        s = lax.rem(i, 2)

        @pl.when(i == 0)
        def _():
            block(dy, 0, 0).start()
            whole(0).start()
            whole(0).wait()

        @pl.when(i + 1 < n)
        def _():
            block(dy, i + 1, 1 - s).start()

        @pl.when((i + 1 >= n) & (i + 1 < 2 * n))
        def _():
            block(x, i + 1 - n, 1 - s).start()

        @pl.when(i == 1)
        def _():
            whole(1).start()
            whole(2).start()

        @pl.when(i < n)
        def _():
            block(dy, i, s).wait()

            def part(h, _):
                for m in range(2):
                    r = pl.ds(pl.multiple_of((2 * h + m) * mt, mt), mt)
                    dwd[r, :] = lax.dot_general(hv[:, r], blk[s], TN, preferred_element_type=f32).astype(bf16)
                return 0

            lax.fori_loop(0, F // mt // 2, part, 0)

        @pl.when(i == n)
        def _():
            whole(1).wait()
            whole(2).wait()

        @pl.when(i >= n)
        def _():
            block(x, i - n, s).wait()

            def part(h, _):
                for src, dst in ((gv, dwg), (uv, dwu)):
                    for m in range(2):
                        c = pl.ds(pl.multiple_of((2 * h + m) * mt, mt), mt)
                        dst[:, c] = lax.dot_general(blk[s], src[:, c], TN, preferred_element_type=f32).astype(bf16)
                return 0

            lax.fori_loop(0, F // mt // 2, part, 0)

    sh = jax.ShapeDtypeStruct
    dma = pltpu.SemaphoreType.DMA
    late = pl.BlockSpec((bw, F), lambda i: (jnp.maximum(i - n, 0), 0))
    return pl.pallas_call(
        kern, grid=(2 * n,), name="weights", in_specs=[pl.BlockSpec(memory_space=pl.ANY)] * 5,
        out_specs=[pl.BlockSpec((F, bw), lambda i: (0, jnp.minimum(i, n - 1))), late, late],
        out_shape=[sh((F, D), bf16), sh((D, F), bf16), sh((D, F), bf16)],
        scratch_shapes=[pltpu.VMEM((T, F), bf16)] * 3 + [pltpu.VMEM((2, T, bw), bf16), dma((3,)), dma((2,))],
        compiler_params=pltpu.CompilerParams(vmem_limit_bytes=62 * 2**20, dimension_semantics=("arbitrary",)),
        cost_estimate=pl.CostEstimate(flops=6 * T * D * F, bytes_accessed=2 * (3 * D * F + 2 * T * D + 3 * T * F), transcendentals=0),
    )


def solution(mesh):
    rows, cols = P(("dp", "tp"), None), P("dp", "tp")
    wcol, wrow = P(None, "tp"), P("tp", None)
    nd = mesh.shape["tp"]

    def body(x, dy, gate, up, w_gate, w_up, w_down):
        T, F, D = gate.shape[0], gate.shape[1], x.shape[1]
        dyr, xr, hid, dg, du, dx = front(nd, T, D, F)(x, dy, gate, up, w_down, w_gate, w_up)
        dx = lax.psum_scatter(dx, "tp", scatter_dimension=0, tiled=True)
        dwd, dwg, dwu = weights(T, D, F)(dyr, xr, hid, dg, du)
        return dx, dwg, dwu, dwd

    return jax.shard_map(
        body, mesh=mesh, in_specs=(rows, rows, cols, cols, wcol, wcol, wrow), out_specs=(rows, cols, cols, rows), check_vma=False)
```
